16 devices in a mesh: rep: 1, dp: 16 (over x, y, z, core).
Axes of the slice: x: 2, y: 2, z: 2, core: 2. Of those that a mesh axis runs over, the one named last changes fastest.
Arguments:
- x: bfloat16 [16, 2048, 1024], P(('rep', 'dp'))
- dy: bfloat16 [16, 2048, 1024], P(('rep', 'dp'))
- w_gate: bfloat16 [2, 1024, 2816], P(None, 'dp')
- w_up: bfloat16 [2, 1024, 2816], P(None, 'dp')
- w_down: bfloat16 [2, 2816, 1024], P(None, 'dp')
Outputs:
- output 1: bfloat16 [16, 2048, 1024], P(('rep', 'dp'))
- output 2: bfloat16 [2, 1024, 2816], P('rep', 'dp')
- output 3: bfloat16 [2, 1024, 2816], P('rep', 'dp')
- output 4: bfloat16 [2, 2816, 1024], P('rep', 'dp')
All inputs are finite; a program needn't handle non-finite values.
Results may differ from the reference program's by a relative error of at most 0.018.
Values are sent between devices in bfloat16 or wider.
A program may use at most 2 GiB of HBM per device.

```python
import jax
import jax.numpy as jnp
from jax import lax

SEQUENCES = 16
TOKENS = 2048
D = 1024
FF = 2816
LAYERS = 2
NAMES = ("w_gate", "w_up", "w_down")
SHAPES = {"w_gate": (LAYERS, D, FF), "w_up": (LAYERS, D, FF), "w_down": (LAYERS, FF, D)}


def bump(key, n, height):
    away = (jnp.arange(n, dtype=jnp.int32) - jax.random.randint(key, (), 0, n, jnp.int32)) % n
    return jnp.where(away < n // 8, height, 1.0)


def together(key, own, strength):
    shared = jax.random.normal(key, own.shape[1:], jnp.float32)
    return (own + strength * shared) * lax.rsqrt(1 + strength * strength)


def setup_inputs(seed: int = 0, part: int = 0) -> dict:
    kx, kdy, ka, kb, kz, kf, kh, kl, *kw = jax.random.split(jax.random.key(seed), 8 + len(NAMES))
    kx, kdy, ka, kb = (jax.random.fold_in(k, part) for k in (kx, kdy, ka, kb))
    shape = (SEQUENCES, TOKENS, D)
    much_x, much_dy = jax.random.uniform(kz, (2,), jnp.float32, 0.0, 1.0)
    layers = 2.0 ** jax.random.uniform(kl, (LAYERS, 1, 1), jnp.float32, -1.0, 1.0)
    x = together(ka, jax.random.normal(kx, shape, jnp.float32), much_x) * bump(kf, D, 4.0)
    dy = together(kb, jax.random.normal(kdy, shape, jnp.float32), much_dy)
    drawn = {"x": x.astype(jnp.bfloat16), "dy": (dy * (SEQUENCES * TOKENS) ** -0.5).astype(jnp.bfloat16)}
    for key, name in zip(kw, NAMES, strict=True):
        w = jax.random.normal(key, SHAPES[name], jnp.float32) * SHAPES[name][1] ** -0.5
        drawn[name] = (w * {"w_gate": 1.0, "w_up": bump(kh, FF, 4.0), "w_down": layers}[name]).astype(jnp.bfloat16)
    return drawn


def matmul(a, w):
    return jnp.dot(a, w, preferred_element_type=jnp.float32).astype(jnp.bfloat16)


def normed(h):
    wide = h.astype(jnp.float32)
    scale = lax.rsqrt(jnp.mean(wide**2, -1, keepdims=True) + 1e-6)
    return (wide * scale).astype(jnp.bfloat16)


def layer(h, w):
    a = normed(h)
    gate = jnp.dot(a, w["w_gate"], preferred_element_type=jnp.float32)
    up = jnp.dot(a, w["w_up"], preferred_element_type=jnp.float32)
    return h + matmul((jax.nn.silu(gate) * up).astype(jnp.bfloat16), w["w_down"])


def stack(weights, h):
    return lax.scan(lambda h, w: (layer(h, w), None), h, weights)[0]


def reference(x, dy, w_gate, w_up, w_down):
    weights = dict(zip(NAMES, (w_gate, w_up, w_down), strict=True))

    def take(so_far, sequence):
        h, by_y = sequence
        _, back = jax.vjp(stack, weights, h)
        by_weights, by_h = back(by_y)
        return jax.tree.map(lambda total, term: total + term.astype(jnp.float32), so_far, by_weights), by_h

    none_yet = {name: jnp.zeros(w.shape, jnp.float32) for name, w in weights.items()}
    by_weights, by_x = lax.scan(take, none_yet, (x, dy))
    return (by_x, *(by_weights[name].astype(jnp.bfloat16) for name in NAMES))
```

```python
import jax
import jax.numpy as jnp
from jax import lax
from jax.sharding import PartitionSpec as P

F32, BF16 = jnp.float32, jnp.bfloat16
EPS = 1e-6


def dot(a, b, dims):
    return lax.dot_general(a, b, (dims, ((), ())), preferred_element_type=F32)


NN, NT, TN = ((1,), (0,)), ((1,), (1,)), ((0,), (0,))


def normed(h):
    wide = h.astype(F32)
    scale = lax.rsqrt(jnp.mean(wide**2, -1, keepdims=True) + EPS)
    return (wide * scale).astype(BF16)


def norm_back(h, da, dy):
    wide, d = h.astype(F32), da.astype(F32)
    scale = lax.rsqrt(jnp.mean(wide**2, -1, keepdims=True) + EPS)
    through = jnp.sum(d * wide, -1, keepdims=True)
    dh = d * scale - wide * (scale**3 * through / h.shape[-1])
    return dy + dh.astype(BF16)


def gated(gate, up):
    return (gate * jax.nn.sigmoid(gate) * up).astype(BF16)


def gated_back(gate, up, dhid):
    d, s = dhid.astype(F32), jax.nn.sigmoid(gate)
    dgate = d * up * (s * (1 + gate * (1 - s)))
    return dgate.astype(BF16), (d * gate * s).astype(BF16)


def gather(w):
    return lax.all_gather(w, "dp", axis=0, tiled=True)


def scatter(g):
    return lax.psum_scatter(g, "dp", scatter_dimension=0, tiled=True)


def device_step(x, dy, w_gate, w_up, w_down):
    x, dy = x[0], dy[0]
    wg0, wu0, wd0 = gather(w_gate[0]), gather(w_up[0]), gather(w_down[0])
    wd1, wg1, wu1 = gather(w_down[1]), gather(w_gate[1]), gather(w_up[1])

    a0 = normed(x)
    gate0, up0 = dot(a0, wg0, NN), dot(a0, wu0, NN)
    hid0 = gated(gate0, up0)
    h1 = x + dot(hid0, wd0, NN).astype(BF16)

    dhid1 = dot(dy, wd1, NT).astype(BF16)
    a1 = normed(h1)
    gate1, up1 = dot(a1, wg1, NN), dot(a1, wu1, NN)
    hid1 = gated(gate1, up1)
    dgate1, dup1 = gated_back(gate1, up1, dhid1)

    gd1 = scatter(dot(hid1, dy, TN).astype(BF16))
    gg1 = scatter(dot(a1, dgate1, TN).astype(BF16))
    gu1 = scatter(dot(a1, dup1, TN).astype(BF16))
    da1 = (dot(dgate1, wg1, NT) + dot(dup1, wu1, NT)).astype(BF16)
    dh1 = norm_back(h1, da1, dy)

    dhid0 = dot(dh1, wd0, NT).astype(BF16)
    dgate0, dup0 = gated_back(gate0, up0, dhid0)
    gd0 = scatter(dot(hid0, dh1, TN).astype(BF16))
    gg0 = scatter(dot(a0, dgate0, TN).astype(BF16))
    gu0 = scatter(dot(a0, dup0, TN).astype(BF16))
    da0 = (dot(dgate0, wg0, NT) + dot(dup0, wu0, NT)).astype(BF16)
    dx = norm_back(x, da0, dh1)
    return dx[None], jnp.stack([gg0, gg1]), jnp.stack([gu0, gu1]), jnp.stack([gd0, gd1])


def solution(mesh):
    tokens, rows = P(("rep", "dp"), None, None), P(None, "dp", None)
    return jax.shard_map(
        device_step,
        mesh=mesh,
        in_specs=(tokens, tokens, rows, rows, rows),
        out_specs=(tokens, P("rep", "dp", None), P("rep", "dp", None), P("rep", "dp", None)),
        check_vma=False,
    )
```

```python
import functools

import jax
import jax.numpy as jnp
from jax import lax
from jax.experimental import pallas as pl
from jax.experimental.pallas import tpu as pltpu
from jax.sharding import PartitionSpec as P

F32, BF16 = jnp.float32, jnp.bfloat16
EPS = 1e-6
VMEM_LIMIT = 66_000_000
ANY = pl.BlockSpec(memory_space=pl.ANY)
BOTH = pl.ds(0, 2)
ORDERS = ((0, 1, 2), (1, 2, 0), (2, 0, 1))
PARTS = {2816: ((0, 1024), (1024, 896), (1920, 896)), 1024: ((0, 384), (384, 384), (768, 256))}
NN, NT, TN = ((1,), (0,)), ((1,), (1,)), ((0,), (0,))


def dot(a, b, dims=NN):
    return lax.dot_general(a, b, (dims, ((), ())), preferred_element_type=F32)


def place():
    i = lax.axis_index("dp")
    return [(i // 8) % 2, (i // 4) % 2, (i // 2) % 2, i % 2]


def peer(axis):
    i, step = lax.axis_index("dp"), 8 >> axis
    return {"dp": i + step * (1 - 2 * ((i // step) % 2))}


def remote(src, dst, send, recv, axis):
    return pltpu.make_async_remote_copy(
        src_ref=src, dst_ref=dst, send_sem=send, recv_sem=recv, device_id=peer(axis), device_id_type=pl.DeviceIdType.MESH
    )


def meet():
    barrier = pltpu.get_barrier_semaphore()
    for axis in range(4):
        pl.semaphore_signal(barrier, inc=1, device_id=peer(axis), device_id_type=pl.DeviceIdType.MESH)
    pl.semaphore_wait(barrier, 4)


class Gather:
    def __init__(self, layer, *blocks):
        n = self.n = len(blocks)
        self.layer, self.inputs = layer, blocks
        shapes = [b.shape[1:] for b in blocks]
        self.cols = [PARTS[s[1]] for s in shapes]
        self.out_shapes = [jax.ShapeDtypeStruct((2, 2, 2, 2, *s), BF16) for s in shapes]
        dma = pltpu.SemaphoreType.DMA
        self.scratch = [pltpu.VMEM(s, BF16) for s in shapes] + [dma((n, 2)), dma((n, 3, 4)), dma((n, 3, 4))]

    def events(self, blocks, wholes, scratch):
        own, (local, send, recv) = scratch[: self.n], scratch[self.n :]
        at = place()
        weights = range(self.n)

        def copy(w, p, stage):
            order, (start, size) = (*ORDERS[p], 3), self.cols[w][p]
            index = tuple(BOTH if a in order[:stage] else at[a] for a in range(4))
            columns = (slice(None), pl.ds(start, size))
            dst = wholes[w].at[(*index, *columns)]
            src = blocks[w].at[(self.layer, *columns)] if stage == 0 else dst
            return remote(src, dst, send.at[w, p, stage], recv.at[w, p, stage], order[stage])

        def take(w):
            return pltpu.make_async_copy(blocks[w].at[self.layer], own[w], local.at[w, 0])

        def put(w):
            return pltpu.make_async_copy(own[w], wholes[w].at[tuple(at)], local.at[w, 1])

        def first():
            for w in weights:
                take(w).start()
                for p in range(3):
                    copy(w, p, 0).start()
            for w in weights:
                take(w).wait()
                put(w).start()

        def later(w, stage):
            if stage == 1:
                put(w).wait()
            for p in range(3):
                copy(w, p, stage - 1).wait_recv()
                copy(w, p, stage).start()

        def last():
            for w in weights:
                for p in range(3):
                    copy(w, p, 3).wait_recv()
                    for stage in range(4):
                        copy(w, p, stage).wait_send()

        middle = [functools.partial(later, w, stage) for stage in (1, 2, 3) for w in weights]
        return [first, *middle, last]


class Scatter:
    def __init__(self, *terms):
        n = self.n = len(terms)
        self.inputs = terms
        shapes = [t.shape[4:] for t in terms]
        self.cols = [PARTS[s[1]] for s in shapes]
        self.rows = [s[0] for s in shapes]
        self.out_shapes = [jax.ShapeDtypeStruct(s, BF16) for s in shapes]
        dma = pltpu.SemaphoreType.DMA
        self.scratch = []
        for s in shapes:
            self.scratch += [pltpu.VMEM((*(2,) * lead, *s), BF16) for lead in (3, 3, 2, 1, 0)]
        self.scratch += [dma((n, 2)), dma((n, 2)), dma((n, 3, 3)), dma((n, 3, 3))]

    def events(self, terms, sums, scratch):
        held = [scratch[5 * w : 5 * w + 5] for w in range(self.n)]
        local, core, send, recv = scratch[5 * self.n :]
        at = place()
        cube = at[:3]
        items = [(w, p) for w in range(self.n) for p in range(3)]

        def swap(w):
            return remote(terms[w].at[BOTH, BOTH, BOTH, 1 - at[3]], held[w][1], core.at[w, 0], core.at[w, 1], 3)

        def take(w):
            return pltpu.make_async_copy(terms[w].at[BOTH, BOTH, BOTH, at[3]], held[w][0], local.at[w, 0])

        def put(w):
            return pltpu.make_async_copy(held[w][0].at[tuple(cube)], sums[w], local.at[w, 1])

        def columns(w, p):
            return pl.ds(*self.cols[w][p])

        def copy(w, p, stage):
            order = ORDERS[p]
            index = list(cube)
            index[order[stage]] = 1 - cube[order[stage]]
            for a in order[stage + 1 :]:
                index[a] = BOTH
            src = held[w][0].at[(*index, slice(None), columns(w, p))]
            dst = held[w][2 + stage].at[(*(BOTH,) * (2 - stage), slice(None), columns(w, p))]
            return remote(src, dst, send.at[w, p, stage], recv.at[w, p, stage], order[stage])

        def add(w, p, stage):
            order = ORDERS[p]
            free = order[stage + 1 :] if stage < 3 else ()
            chunk = 32 if self.rows[w] % 32 == 0 else 16
            for number in range(2 ** len(free)):
                index = list(cube)
                if stage < 3:
                    index[order[stage]] = 1 - cube[order[stage]]
                for k, a in enumerate(free):
                    index[a] = (number >> k) & 1

                def some_rows(i, index=index):
                    where = (pl.ds(pl.multiple_of(i * chunk, chunk), chunk), columns(w, p))
                    total = held[w][0][(*index, *where)].astype(F32) + held[w][1][(*index, *where)].astype(F32)
                    for j in range(stage):
                        rest = [index[a] for a in range(3) if a not in order[: j + 1]]
                        total += held[w][2 + j][(*rest, *where)].astype(F32)
                    held[w][0][(*index, *where)] = total.astype(BF16)

                pl.loop(0, self.rows[w] // chunk)(some_rows)

        def first():
            for w in range(self.n):
                swap(w).start()
                take(w).start()

        def leave(w, stage):
            if stage == 0:
                take(w).wait()
                swap(w).wait_recv()
            for p in range(3):
                if stage > 0:
                    copy(w, p, stage - 1).wait_recv()
                add(w, p, stage)
                if stage < 3:
                    copy(w, p, stage).start()
            if stage == 3:
                put(w).start()

        def last():
            for w in range(self.n):
                swap(w).wait_send()
                for p in range(3):
                    for stage in range(3):
                        copy(w, p, stage).wait_send()
                put(w).wait()

        middle = [functools.partial(leave, w, stage) for stage in range(4) for w in range(self.n)]
        return [first, *middle, last]


def call(name, body, steps, inputs, in_specs, out_shapes, out_specs, flops=0, scratch=(), side=None, when=(), number=None):
    n_in, n_out, n_scratch = len(inputs), len(out_shapes), len(scratch)
    s_in, s_out = (len(side.inputs), len(side.out_shapes)) if side else (0, 0)

    def kernel(*refs):
        ins, refs = refs[:n_in], refs[n_in:]
        side_ins, refs = refs[:s_in], refs[s_in:]
        outs, refs = refs[:n_out], refs[n_out:]
        side_outs, refs = refs[:s_out], refs[s_out:]
        own, side_scratch = refs[:n_scratch], refs[n_scratch:]
        step = pl.program_id(0)
        events = side.events(side_ins, side_outs, side_scratch) if side else []
        for k, event in enumerate(events):
            if k < len(when):

                def now(event=event, k=k):
                    if k == 0:
                        meet()
                    event()

                pl.when(step == when[k])(now)
        body(*ins, *outs, *own)
        if len(events) > len(when):

            def end():
                for event in events[len(when) :]:
                    event()

            pl.when(step == steps - 1)(end)

    params = dict(vmem_limit_bytes=VMEM_LIMIT, dimension_semantics=("arbitrary",))
    if side:
        params |= dict(collective_id=number, has_side_effects=True)
    return pl.pallas_call(
        kernel,
        name=name,
        grid=(steps,),
        in_specs=[*in_specs, *[ANY] * s_in],
        out_specs=[*out_specs, *[ANY] * s_out],
        out_shape=[*out_shapes, *(side.out_shapes if side else ())],
        scratch_shapes=[*scratch, *(side.scratch if side else ())],
        compiler_params=pltpu.CompilerParams(**params),
        cost_estimate=pl.CostEstimate(flops=flops, bytes_accessed=0, transcendentals=0),
    )(*inputs, *(side.inputs if side else ()))


def shape(*dims, dtype=BF16):
    return jax.ShapeDtypeStruct(dims, dtype)


def kept(*dims):
    return pl.BlockSpec(dims, lambda i: (0,) * len(dims), pipeline_mode=pl.Buffered(1))


def across(rows, size):
    return pl.BlockSpec((rows, size), lambda i: (0, i))


def down(size, cols):
    return pl.BlockSpec((size, cols), lambda i: (i, 0))


T, D, FF = 2048, 1024, 2816
MM = 2 * T * D * FF


def scale_of(wide):
    return lax.rsqrt(jnp.mean(wide**2, -1, keepdims=True) + EPS)


def normed(wide):
    return (wide * scale_of(wide)).astype(BF16)


def norm_body(x, a, at):
    wide = x[...].astype(F32)
    y = wide * scale_of(wide)
    a[...] = y.astype(BF16)
    at[...] = y.T.astype(BF16)


def norm(x, **side):
    n = 256
    return call("norm", norm_body, T // n, [x], [down(n, D)], [shape(T, D), shape(D, T)], [down(n, D), across(D, n)], **side)


def chunks(n=512):
    return [pl.ds(r, n) for r in range(0, T, n)]


def gate_up_body(a, wg, wu, gate, up, hid):
    for r in chunks():
        g, u = dot(a[r, :], wg[...]), dot(a[r, :], wu[...])
        gate[r, :], up[r, :] = g, u
        hid[r, :] = (g * jax.nn.sigmoid(g) * u).astype(BF16)


def gate_up(a, wg, wu, **side):
    n = 256
    wide = shape(T, FF, dtype=F32)
    return call(
        "gate_up", gate_up_body, FF // n, [a, wg, wu], [kept(T, D), across(D, n), across(D, n)],
        [wide, wide, shape(T, FF)], [across(T, n)] * 3, flops=2 * MM, **side,
    )


def down_body(hid, wd, x, h, a, at):
    y = x[...] + dot(hid[...], wd[...]).astype(BF16)
    h[...] = y
    wide = y.astype(F32)
    y = wide * scale_of(wide)
    a[...] = y.astype(BF16)
    at[...] = y.T.astype(BF16)


def down_norm(hid, wd, x, **side):
    n = 256
    return call(
        "down", down_body, T // n, [hid, wd, x], [down(n, FF), kept(FF, D), down(n, D)],
        [shape(T, D), shape(T, D), shape(D, T)], [down(n, D), down(n, D), across(D, n)], flops=MM, **side,
    )


def gated_back(g, u, d):
    s = jax.nn.sigmoid(g)
    gs = g * s
    return (d * u * (s + gs * (1 - s))).astype(BF16), (d * gs).astype(BF16), (gs * u).astype(BF16)


def turn_body(a, dy, wg, wu, wd, hid, dgate, dup):
    for r in chunks(256):
        g, u = dot(a[r, :], wg[...]), dot(a[r, :], wu[...])
        d = dot(dy[r, :], wd[...], NT).astype(BF16).astype(F32)
        dgate[r, :], dup[r, :], hid[r, :] = gated_back(g, u, d)


def turn(a, dy, wg, wu, wd, **side):
    n = 256
    return call(
        "turn", turn_body, FF // n, [a, dy, wg, wu, wd],
        [kept(T, D), kept(T, D), across(D, n), across(D, n), down(n, D)],
        [shape(T, FF)] * 3, [across(T, n)] * 3, flops=3 * MM, **side,
    )


def hidden_back_body(dh, wd, gate, up, dgate, dup):
    for r in chunks(256):
        d = dot(dh[r, :], wd[...], NT).astype(BF16).astype(F32)
        dgate[r, :], dup[r, :], _ = gated_back(gate[r, :], up[r, :], d)


def hidden_back(dh, wd, gate, up, **side):
    n = 256
    return call(
        "hidden_back", hidden_back_body, FF // n, [dh, wd, gate, up],
        [kept(T, D), down(n, D), across(T, n), across(T, n)], [shape(T, FF)] * 2, [across(T, n)] * 2, flops=MM, **side,
    )


def grad_down_body(hid, dy, out):
    out[...] = dot(hid[...], dy[...], TN).astype(BF16)


def grad_down(hid, dy, **side):
    n = 256
    return call("grad_down", grad_down_body, FF // n, [hid, dy], [across(T, n), kept(T, D)], [shape(FF, D)], [down(n, D)], flops=MM, **side)


def grad_in_body(at, d, out):
    out[...] = dot(at[...], d[...]).astype(BF16)


def grad_in(at, d, **side):
    n = 256
    return call("grad_in", grad_in_body, FF // n, [at, d], [kept(D, T), across(T, n)], [shape(D, FF)], [across(D, n)], flops=MM, **side)


def back_body(dg, du, wg, wu, h, dy, out):
    da = (dot(dg[...], wg[...], NT) + dot(du[...], wu[...], NT)).astype(BF16).astype(F32)
    wide = h[...].astype(F32)
    s = scale_of(wide)
    through = jnp.sum(da * wide, -1, keepdims=True)
    out[...] = dy[...] + (da * s - wide * (s * s * s * through / D)).astype(BF16)


def back(dg, du, wg, wu, h, dy, **side):
    n = 256
    return call(
        "back", back_body, T // n, [dg, du, wg, wu, h, dy],
        [down(n, FF), down(n, FF), kept(D, FF), kept(D, FF), down(n, D), down(n, D)],
        [shape(T, D)], [down(n, D)], flops=2 * MM, **side,
    )


def blocks_of(grad):
    return grad.reshape(2, 2, 2, 2, -1, grad.shape[-1])


def device_step(x, dy, w_gate, w_up, w_down):
    x, dy = x.reshape(T, D), dy.reshape(T, D)

    a0, a0t, wg0, wu0, wd0 = norm(x, side=Gather(0, w_gate, w_up, w_down), when=(0, 2, 3, 4), number=1)
    wg0, wu0, wd0 = wg0.reshape(D, FF), wu0.reshape(D, FF), wd0.reshape(FF, D)
    gate0, up0, hid0, wg1, wu1 = gate_up(a0, wg0, wu0, side=Gather(1, w_gate, w_up), when=(0, 1, 2, 4, 6, 10), number=2)
    h1, a1, a1t, wd1 = down_norm(hid0, wd0, x, side=Gather(1, w_down), when=(0, 2, 4), number=3)
    wg1, wu1, wd1 = wg1.reshape(D, FF), wu1.reshape(D, FF), wd1.reshape(FF, D)

    hid1, dgate1, dup1 = turn(a1, dy, wg1, wu1, wd1)
    (gd1,) = grad_down(hid1, dy)
    gg1, sd1 = grad_in(a1t, dgate1, side=Scatter(blocks_of(gd1)), when=(0, 4), number=4)
    (gu1,) = grad_in(a1t, dup1)
    dh1, sg1, su1 = back(dgate1, dup1, wg1, wu1, h1, dy, side=Scatter(blocks_of(gg1), blocks_of(gu1)), when=(0, 2, 3, 5, 7), number=5)

    (gd0,) = grad_down(hid0, dh1)
    dgate0, dup0, sd0 = hidden_back(dh1, wd0, gate0, up0, side=Scatter(blocks_of(gd0)), when=(0, 3, 6, 9), number=6)
    (gg0,) = grad_in(a0t, dgate0)
    gu0, sg0 = grad_in(a0t, dup0, side=Scatter(blocks_of(gg0)), when=(0, 4), number=7)
    dx, su0 = back(dgate0, dup0, wg0, wu0, x, dh1, side=Scatter(blocks_of(gu0)), when=(0, 2, 5, 7), number=8)
    return dx[None], jnp.stack([sg0, sg1]), jnp.stack([su0, su1]), jnp.stack([sd0, sd1])


def solution(mesh):
    tokens, rows = P(("rep", "dp"), None, None), P(None, "dp", None)
    return jax.shard_map(
        device_step,
        mesh=mesh,
        in_specs=(tokens, tokens, rows, rows, rows),
        out_specs=(tokens, P("rep", "dp", None), P("rep", "dp", None), P("rep", "dp", None)),
        check_vma=False,
    )
```

```python
import functools

import jax
import jax.numpy as jnp
from jax import lax
from jax.experimental import pallas as pl
from jax.experimental.pallas import tpu as pltpu
from jax.sharding import PartitionSpec as P

F32, BF16 = jnp.float32, jnp.bfloat16
EPS = 1e-6
VMEM_LIMIT = 66_000_000
ANY = pl.BlockSpec(memory_space=pl.ANY)
BOTH = pl.ds(0, 2)
ORDERS = ((0, 1, 2), (1, 2, 0), (2, 0, 1))
PARTS = {
    2816: ((0, 1024), (1024, 896), (1920, 896)),
    1536: ((0, 512), (512, 512), (1024, 512)),
    1280: ((0, 512), (512, 384), (896, 384)),
    1024: ((0, 384), (384, 384), (768, 256)),
}
NN, NT, TN = ((1,), (0,)), ((1,), (1,)), ((0,), (0,))


def dot(a, b, dims=NN):
    return lax.dot_general(a, b, (dims, ((), ())), preferred_element_type=F32)


def place():
    i = lax.axis_index("dp")
    return [(i // 8) % 2, (i // 4) % 2, (i // 2) % 2, i % 2]


def peer(axis):
    i, step = lax.axis_index("dp"), 8 >> axis
    return {"dp": i + step * (1 - 2 * ((i // step) % 2))}


def remote(src, dst, send, recv, axis):
    return pltpu.make_async_remote_copy(
        src_ref=src, dst_ref=dst, send_sem=send, recv_sem=recv, device_id=peer(axis), device_id_type=pl.DeviceIdType.MESH
    )


def meet():
    barrier = pltpu.get_barrier_semaphore()
    for axis in range(4):
        pl.semaphore_signal(barrier, inc=1, device_id=peer(axis), device_id_type=pl.DeviceIdType.MESH)
    pl.semaphore_wait(barrier, 4)


class Gather:
    def __init__(self, *weights):
        n = self.n = len(weights)
        self.inputs, self.layers, self.starts, sizes, self.shifts = zip(*weights)
        shapes = [(b.shape[1], size) for b, size in zip(self.inputs, sizes)]
        self.cols = [PARTS[size] for size in sizes]
        self.out_shapes = [jax.ShapeDtypeStruct((2, 2, 2, 2, *s), BF16) for s in shapes]
        dma = pltpu.SemaphoreType.DMA
        self.scratch = [pltpu.VMEM(s, BF16) for s in shapes] + [dma((n, 2)), *[dma((n, 3, k)) for k in (3, 3, 4, 4)]]

    def events(self, blocks, wholes, scratch):
        own, (local, send, recv, relay_send, relay_recv) = scratch[: self.n], scratch[self.n :]
        at = place()
        weights = range(self.n)

        def part(w, p, index):
            start, size = self.cols[w][p]
            return wholes[w].at[(*index, slice(None), pl.ds(start, size))]

        def block(w, p):
            start, size = self.cols[w][p]
            return blocks[w].at[(self.layers[w], slice(None), pl.ds(self.starts[w] + start, size))]

        def copy(w, p, stage):
            order = ORDERS[(p + self.shifts[w]) % 3]
            dst = part(w, p, [BOTH if a in order[:stage] else at[a] for a in range(4)])
            return remote(dst if stage else block(w, p), dst, send.at[w, p, stage], recv.at[w, p, stage], order[stage])

        def relay(w, p, stage):
            index, order = list(at), ORDERS[(p + self.shifts[w]) % 3]
            if stage:
                index[order[stage - 1]] = 1 - at[order[stage - 1]]
                for a in order[: stage - 1]:
                    index[a] = BOTH
            dst = part(w, p, index)
            return remote(dst if stage else block(w, p), dst, relay_send.at[w, p, stage], relay_recv.at[w, p, stage], 3)

        def take(w):
            block = blocks[w].at[(self.layers[w], slice(None), pl.ds(self.starts[w], own[w].shape[1]))]
            return pltpu.make_async_copy(block, own[w], local.at[w, 0])

        def put(w):
            return pltpu.make_async_copy(own[w], wholes[w].at[tuple(at)], local.at[w, 1])

        def first():
            for w in weights:
                take(w).start()
                for p in range(3):
                    copy(w, p, 0).start()
            for w in weights:
                for p in range(3):
                    relay(w, p, 0).start()
                take(w).wait()
                put(w).start()

        def later(w, stage):
            if stage == 1:
                put(w).wait()
            for p in range(3):
                copy(w, p, stage - 1).wait_recv()
                if stage < 3:
                    copy(w, p, stage).start()
                relay(w, p, stage).start()

        def last():
            for w in weights:
                for p in range(3):
                    for stage in range(4):
                        relay(w, p, stage).wait_recv()
                        relay(w, p, stage).wait_send()
                        if stage < 3:
                            copy(w, p, stage).wait_send()

        middle = [functools.partial(later, w, stage) for stage in (1, 2, 3) for w in weights]
        return [first, *middle, last]


class Scatter:
    def __init__(self, *terms):
        n = self.n = len(terms)
        terms, self.shifts = zip(*terms)
        self.inputs = terms
        shapes = [t.shape[4:] for t in terms]
        self.cols = [PARTS[s[1]] for s in shapes]
        self.rows = [s[0] for s in shapes]
        self.out_shapes = [jax.ShapeDtypeStruct(s, BF16) for s in shapes]
        dma = pltpu.SemaphoreType.DMA
        self.scratch = []
        for s in shapes:
            self.scratch += [pltpu.VMEM((*(2,) * lead, *s), BF16) for lead in (3, 3, 2, 1, 0)]
        self.scratch += [dma((n, 2)), dma((n, 3, 4)), dma((n, 3, 3)), dma((n, 3, 3))]

    def order(self, w, p):
        return ORDERS[(p + self.shifts[w]) % 3]

    def events(self, terms, sums, scratch):
        held = [scratch[5 * w : 5 * w + 5] for w in range(self.n)]
        local, core, send, recv = scratch[5 * self.n :]
        at = place()
        cube = at[:3]
        items = [(w, p) for w in range(self.n) for p in range(3)]

        def swap(w, p, near):
            first = self.order(w, p)[0]
            index = [BOTH, BOTH, BOTH]
            index[first] = cube[first] if near else 1 - cube[first]
            src = terms[w].at[(*index, 1 - at[3], slice(None), columns(w, p))]
            dst = held[w][1].at[(*index, slice(None), columns(w, p))]
            return remote(src, dst, core.at[w, p, 2 * near], core.at[w, p, 2 * near + 1], 3)

        def take(w):
            return pltpu.make_async_copy(terms[w].at[BOTH, BOTH, BOTH, at[3]], held[w][0], local.at[w, 0])

        def put(w):
            return pltpu.make_async_copy(held[w][0].at[tuple(cube)], sums[w], local.at[w, 1])

        def columns(w, p):
            return pl.ds(*self.cols[w][p])

        def copy(w, p, stage):
            order = self.order(w, p)
            index = list(cube)
            index[order[stage]] = 1 - cube[order[stage]]
            for a in order[stage + 1 :]:
                index[a] = BOTH
            src = held[w][0].at[(*index, slice(None), columns(w, p))]
            dst = held[w][2 + stage].at[(*(BOTH,) * (2 - stage), slice(None), columns(w, p))]
            return remote(src, dst, send.at[w, p, stage], recv.at[w, p, stage], order[stage])

        def add(w, p, stage):
            order = self.order(w, p)
            free = order[stage + 1 :] if stage < 3 else ()
            chunk = 32 if self.rows[w] % 32 == 0 else 16
            for number in range(2 ** len(free)):
                index = list(cube)
                if stage < 3:
                    index[order[stage]] = 1 - cube[order[stage]]
                for k, a in enumerate(free):
                    index[a] = (number >> k) & 1

                def some_rows(i, index=index):
                    where = (pl.ds(pl.multiple_of(i * chunk, chunk), chunk), columns(w, p))
                    total = held[w][0][(*index, *where)].astype(F32) + held[w][1][(*index, *where)].astype(F32)
                    for j in range(stage):
                        rest = [index[a] for a in range(3) if a not in order[: j + 1]]
                        total += held[w][2 + j][(*rest, *where)].astype(F32)
                    held[w][0][(*index, *where)] = total.astype(BF16)

                pl.loop(0, self.rows[w] // chunk)(some_rows)

        def first():
            for near in (0, 1):
                for w in range(self.n):
                    for p in range(3):
                        swap(w, p, near).start()
                    if not near:
                        take(w).start()

        def leave(w, stage):
            if stage == 0:
                take(w).wait()
            for p in range(3):
                if stage < 2:
                    swap(w, p, stage).wait_recv()
                if stage > 0:
                    copy(w, p, stage - 1).wait_recv()
                add(w, p, stage)
                if stage < 3:
                    copy(w, p, stage).start()
            if stage == 3:
                put(w).start()

        def last():
            for w in range(self.n):
                for p in range(3):
                    swap(w, p, 0).wait_send()
                    swap(w, p, 1).wait_send()
                    for stage in range(3):
                        copy(w, p, stage).wait_send()
                put(w).wait()

        middle = [functools.partial(leave, w, stage) for stage in range(4) for w in range(self.n)]
        return [first, *middle, last]


def call(name, body, steps, inputs, in_specs, out_shapes, out_specs, flops=0, scratch=(), aliases=None, side=None, when=(), number=None):
    n_in, n_out, n_scratch = len(inputs), len(out_shapes), len(scratch)
    s_in, s_out = (len(side.inputs), len(side.out_shapes)) if side else (0, 0)

    def kernel(*refs):
        ins, refs = refs[:n_in], refs[n_in:]
        side_ins, refs = refs[:s_in], refs[s_in:]
        outs, refs = refs[:n_out], refs[n_out:]
        side_outs, refs = refs[:s_out], refs[s_out:]
        own, side_scratch = refs[:n_scratch], refs[n_scratch:]
        step = pl.program_id(0)
        events = side.events(side_ins, side_outs, side_scratch) if side else []
        for k, event in enumerate(events):
            if k < len(when):

                def now(event=event, k=k):
                    if k == 0:
                        meet()
                    event()

                pl.when(step == when[k])(now)
        body(*ins, *outs, *own)
        if len(events) > len(when):

            def end():
                for event in events[len(when) :]:
                    event()

            pl.when(step == steps - 1)(end)

    params = dict(vmem_limit_bytes=VMEM_LIMIT, dimension_semantics=("arbitrary",))
    if side:
        params |= dict(collective_id=number, has_side_effects=True)
    return pl.pallas_call(
        kernel,
        name=name,
        grid=(steps,),
        in_specs=[*in_specs, *[ANY] * s_in],
        out_specs=[*out_specs, *[ANY] * s_out],
        out_shape=[*out_shapes, *(side.out_shapes if side else ())],
        scratch_shapes=[*scratch, *(side.scratch if side else ())],
        input_output_aliases=aliases or {},
        compiler_params=pltpu.CompilerParams(**params),
        cost_estimate=pl.CostEstimate(flops=flops, bytes_accessed=0, transcendentals=0),
    )(*inputs, *(side.inputs if side else ()))


def shape(*dims, dtype=BF16):
    return jax.ShapeDtypeStruct(dims, dtype)


def kept(*dims):
    return pl.BlockSpec(dims, lambda i: (0,) * len(dims), pipeline_mode=pl.Buffered(1))


def across(rows, size):
    return pl.BlockSpec((rows, size), lambda i: (0, i))


def down(size, cols):
    return pl.BlockSpec((size, cols), lambda i: (i, 0))


T, D, FF = 2048, 1024, 2816
MM = 2 * T * D * FF


def scale_of(wide):
    return lax.rsqrt(jnp.mean(wide**2, -1, keepdims=True) + EPS)


def normed(wide):
    return (wide * scale_of(wide)).astype(BF16)


def norm_body(x, a, at):
    wide = x[...].astype(F32)
    y = wide * scale_of(wide)
    a[...] = y.astype(BF16)
    at[...] = y.T.astype(BF16)


def norm(x, **side):
    n = 256
    return call("norm", norm_body, T // n, [x], [down(n, D)], [shape(T, D), shape(D, T)], [down(n, D), across(D, n)], **side)


def chunks(n=512):
    return [pl.ds(r, n) for r in range(0, T, n)]


def gate_up_body(a, wg, wu, gate, up, hid):
    for r in chunks():
        g, u = dot(a[r, :], wg[...]), dot(a[r, :], wu[...])
        gate[r, :], up[r, :] = g, u
        hid[r, :] = (g * jax.nn.sigmoid(g) * u).astype(BF16)


def gate_up(a, wg, wu, **side):
    n = 256
    wide = shape(T, FF, dtype=F32)
    return call(
        "gate_up", gate_up_body, FF // n, [a, wg, wu], [kept(T, D), across(D, n), across(D, n)],
        [wide, wide, shape(T, FF)], [across(T, n)] * 3, flops=2 * MM, **side,
    )


def down_body(hid, wd, x, h, a, at):
    y = x[...] + dot(hid[...], wd[...]).astype(BF16)
    h[...] = y
    wide = y.astype(F32)
    y = wide * scale_of(wide)
    a[...] = y.astype(BF16)
    at[...] = y.T.astype(BF16)


def down_norm(hid, wd, x, **side):
    n = 256
    return call(
        "down", down_body, T // n, [hid, wd, x], [down(n, FF), kept(FF, D), down(n, D)],
        [shape(T, D), shape(T, D), shape(D, T)], [down(n, D), down(n, D), across(D, n)], flops=MM, **side,
    )


def gated_back(g, u, d):
    s = jax.nn.sigmoid(g)
    gs = g * s
    return (d * u * (s + gs * (1 - s))).astype(BF16), (d * gs).astype(BF16), (gs * u).astype(BF16)


def grads(r_at, r_dy, dgate, dup, hid, gd, gg, gu):
    gg[...] = dot(r_at[...], dgate[...]).astype(BF16)
    gu[...] = dot(r_at[...], dup[...]).astype(BF16)
    gd[...] = dot(hid[...], r_dy[...], TN).astype(BF16)


def turn_body(a, at, dy, wg, wu, wd, *refs):
    dgate, dup, gd, gg, gu, hid = refs[-6:]
    for r in chunks(256):
        g, u = dot(a[r, :], wg[...]), dot(a[r, :], wu[...])
        d = dot(dy[r, :], wd[...], NT).astype(BF16).astype(F32)
        dgate[r, :], dup[r, :], hid[r, :] = gated_back(g, u, d)
    grads(at, dy, dgate, dup, hid, gd, gg, gu)


def turn(a, at, dy, wg, wu, wd, first, tiles, so_far=(), **side):
    n = 256
    columns = pl.BlockSpec((T, n), lambda i: (0, first + i))
    rows = pl.BlockSpec((n, D), lambda i: (first + i, 0))
    return call(
        f"turn_{first}", turn_body, tiles, [a, at, dy, wg, wu, wd, *so_far],
        [kept(T, D), kept(D, T), kept(T, D), across(D, n), across(D, n), rows, *[ANY] * len(so_far)],
        [shape(T, FF), shape(T, FF), shape(FF, D), shape(D, tiles * n), shape(D, tiles * n)],
        [columns, columns, rows, across(D, n), across(D, n)],
        flops=6 * MM * tiles // 11, scratch=[pltpu.VMEM((T, n), BF16)],
        aliases={6 + k: k for k in range(len(so_far))}, **side,
    )


def hidden_back_body(at, dh, wd, gate, up, *refs):
    dgate, dup, gd, gg, gu, hid = refs[-6:]
    for r in chunks(256):
        d = dot(dh[r, :], wd[...], NT).astype(BF16).astype(F32)
        dgate[r, :], dup[r, :], hid[r, :] = gated_back(gate[r, :], up[r, :], d)
    grads(at, dh, dgate, dup, hid, gd, gg, gu)


def hidden_back(at, dh, wd, gate, up, first, tiles, so_far=(), **side):
    n = 256
    columns = pl.BlockSpec((T, n), lambda i: (0, first + i))
    rows = pl.BlockSpec((n, D), lambda i: (first + i, 0))
    return call(
        f"hidden_back_{first}", hidden_back_body, tiles, [at, dh, wd, gate, up, *so_far],
        [kept(D, T), kept(T, D), rows, columns, columns, *[ANY] * len(so_far)],
        [shape(T, FF), shape(T, FF), shape(FF, D), shape(D, tiles * n), shape(D, tiles * n)],
        [columns, columns, rows, across(D, n), across(D, n)],
        flops=4 * MM * tiles // 11, scratch=[pltpu.VMEM((T, n), BF16)],
        aliases={5 + k: k for k in range(len(so_far))}, **side,
    )


def back_body(dg, du, h, dy, *refs):
    *weights, out = refs
    half, start, da = len(weights) // 2, 0, 0
    for wg, wu in zip(weights[:half], weights[half:]):
        k = slice(start, start + wg.shape[1])
        da += dot(dg[:, k], wg[...], NT) + dot(du[:, k], wu[...], NT)
        start += wg.shape[1]
    da = da.astype(BF16).astype(F32)
    wide = h[...].astype(F32)
    s = scale_of(wide)
    through = jnp.sum(da * wide, -1, keepdims=True)
    out[...] = dy[...] + (da * s - wide * (s * s * s * through / D)).astype(BF16)


def back(dg, du, wg, wu, h, dy, **side):
    n = 256
    weights = [*wg, *wu]
    return call(
        "back", back_body, T // n, [dg, du, h, dy, *weights],
        [down(n, FF), down(n, FF), down(n, D), down(n, D), *[kept(*w.shape) for w in weights]],
        [shape(T, D)], [down(n, D)], flops=2 * MM, **side,
    )


def blocks_of(grad):
    return grad.reshape(2, 2, 2, 2, -1, grad.shape[-1])


def device_step(x, dy, w_gate, w_up, w_down):
    x, dy = x.reshape(T, D), dy.reshape(T, D)

    first, rest = 1536, 1280
    a0, a0t, wg0, wu0 = norm(x, side=Gather((w_gate, 0, 0, FF, 0), (w_up, 0, 0, FF, 1)), when=(0, 3, 5), number=1)
    wg0, wu0 = wg0.reshape(D, FF), wu0.reshape(D, FF)
    gate0, up0, hid0, wd0, wd1 = gate_up(
        a0, wg0, wu0, side=Gather((w_down, 0, 0, D, 0), (w_down, 1, 0, D, 1)), when=(0, 2, 2, 4, 6, 10), number=2
    )
    wd0, wd1 = wd0.reshape(FF, D), wd1.reshape(FF, D)
    h1, a1, a1t, wg1a, wu1a = down_norm(
        hid0, wd0, x, side=Gather((w_gate, 1, 0, first, 0), (w_up, 1, 0, first, 1)), when=(0, 2, 2, 4, 5), number=3
    )
    wg1a, wu1a = wg1a.reshape(D, first), wu1a.reshape(D, first)

    *so_far, gg1a, gu1a, wg1b, wu1b = turn(
        a1, a1t, dy, wg1a, wu1a, wd1, 0, 6,
        side=Gather((w_gate, 1, first, rest, 0), (w_up, 1, first, rest, 1)), when=(0, 1, 1, 2, 2, 4, 4, 5), number=4,
    )
    wg1b, wu1b = wg1b.reshape(D, rest), wu1b.reshape(D, rest)
    dgate1, dup1, gd1, gg1b, gu1b, sg1a, su1a = turn(
        a1, a1t, dy, wg1b, wu1b, wd1, 6, 5, so_far,
        side=Scatter((blocks_of(gg1a), 0), (blocks_of(gu1a), 1)), when=(0, 1, 1, 3, 3, 4, 4), number=5,
    )
    dh1, sd1 = back(
        dgate1, dup1, [wg1a, wg1b], [wu1a, wu1b], h1, dy, side=Scatter((blocks_of(gd1), 0)), when=(0, 1, 4, 6, 7), number=6
    )
    *so_far, gg0a, gu0a, sg1b, su1b = hidden_back(
        a0t, dh1, wd0, gate0, up0, 0, 6,
        side=Scatter((blocks_of(gg1b), 0), (blocks_of(gu1b), 1)), when=(0, 1, 1, 3, 3, 4, 4, 5, 5), number=7,
    )
    dgate0, dup0, gd0, gg0b, gu0b, sg0a, su0a = hidden_back(
        a0t, dh1, wd0, gate0, up0, 6, 5, so_far,
        side=Scatter((blocks_of(gg0a), 0), (blocks_of(gu0a), 1)), when=(0, 1, 1, 3, 3, 4, 4), number=8,
    )
    dx, sd0, sg0b, su0b = back(
        dgate0, dup0, [wg0], [wu0], x, dh1,
        side=Scatter((blocks_of(gd0), 0), (blocks_of(gg0b), 2), (blocks_of(gu0b), 2)), when=(0, 1, 2, 2, 5, 6, 7), number=9,
    )
    sg = jnp.stack([jnp.concatenate(pair, 1) for pair in ((sg0a, sg0b), (sg1a, sg1b))])
    su = jnp.stack([jnp.concatenate(pair, 1) for pair in ((su0a, su0b), (su1a, su1b))])
    return dx[None], sg, su, jnp.stack([sd0, sd1])


def solution(mesh):
    tokens, rows = P(("rep", "dp"), None, None), P(None, "dp", None)
    return jax.shard_map(
        device_step,
        mesh=mesh,
        in_specs=(tokens, tokens, rows, rows, rows),
        out_specs=(tokens, P("rep", "dp", None), P("rep", "dp", None), P("rep", "dp", None)),
        check_vma=False,
    )
```

```python
import functools

import jax
import jax.numpy as jnp
from jax import lax
from jax.experimental import pallas as pl
from jax.experimental.pallas import tpu as pltpu
from jax.sharding import PartitionSpec as P

F32, BF16 = jnp.float32, jnp.bfloat16
EPS = 1e-6
VMEM_LIMIT = 66_000_000
ANY = pl.BlockSpec(memory_space=pl.ANY)
BOTH = pl.ds(0, 2)
ORDERS = ((0, 1, 2), (1, 2, 0), (2, 0, 1))
PARTS = {
    2816: ((0, 1024), (1024, 896), (1920, 896)),
    1536: ((0, 512), (512, 512), (1024, 512)),
    1280: ((0, 512), (512, 384), (896, 384)),
    1024: ((0, 384), (384, 384), (768, 256)),
}
NN, NT, TN = ((1,), (0,)), ((1,), (1,)), ((0,), (0,))


def dot(a, b, dims=NN):
    return lax.dot_general(a, b, (dims, ((), ())), preferred_element_type=F32)


def place():
    i = lax.axis_index("dp")
    return [(i // 8) % 2, (i // 4) % 2, (i // 2) % 2, i % 2]


def peer(axis):
    i, step = lax.axis_index("dp"), 8 >> axis
    return {"dp": i + step * (1 - 2 * ((i // step) % 2))}


def remote(src, dst, send, recv, axis):
    return pltpu.make_async_remote_copy(
        src_ref=src, dst_ref=dst, send_sem=send, recv_sem=recv, device_id=peer(axis), device_id_type=pl.DeviceIdType.MESH
    )


def meet():
    barrier = pltpu.get_barrier_semaphore()
    for axis in range(4):
        pl.semaphore_signal(barrier, inc=1, device_id=peer(axis), device_id_type=pl.DeviceIdType.MESH)
    pl.semaphore_wait(barrier, 4)


class Gather:
    aliases = {}


    def __init__(self, *weights):
        n = self.n = len(weights)
        self.inputs, self.layers, self.starts, sizes, self.shifts = zip(*weights)
        shapes = [(b.shape[1], size) for b, size in zip(self.inputs, sizes)]
        self.cols = [PARTS[size] for size in sizes]
        self.out_shapes = [jax.ShapeDtypeStruct((2, 2, 2, 2, *s), BF16) for s in shapes]
        dma = pltpu.SemaphoreType.DMA
        self.scratch = [pltpu.VMEM(s, BF16) for s in shapes] + [dma((n, 2)), *[dma((n, 3, k)) for k in (3, 3, 4, 4)]]

    def events(self, blocks, wholes, scratch):
        own, (local, send, recv, relay_send, relay_recv) = scratch[: self.n], scratch[self.n :]
        at = place()
        weights = range(self.n)

        def part(w, p, index):
            start, size = self.cols[w][p]
            return wholes[w].at[(*index, slice(None), pl.ds(start, size))]

        def block(w, p):
            start, size = self.cols[w][p]
            return blocks[w].at[(self.layers[w], slice(None), pl.ds(self.starts[w] + start, size))]

        def copy(w, p, stage):
            order = ORDERS[(p + self.shifts[w]) % 3]
            dst = part(w, p, [BOTH if a in order[:stage] else at[a] for a in range(4)])
            return remote(dst if stage else block(w, p), dst, send.at[w, p, stage], recv.at[w, p, stage], order[stage])

        def relay(w, p, stage):
            index, order = list(at), ORDERS[(p + self.shifts[w]) % 3]
            if stage:
                index[order[stage - 1]] = 1 - at[order[stage - 1]]
                for a in order[: stage - 1]:
                    index[a] = BOTH
            dst = part(w, p, index)
            return remote(dst if stage else block(w, p), dst, relay_send.at[w, p, stage], relay_recv.at[w, p, stage], 3)

        def take(w):
            block = blocks[w].at[(self.layers[w], slice(None), pl.ds(self.starts[w], own[w].shape[1]))]
            return pltpu.make_async_copy(block, own[w], local.at[w, 0])

        def put(w):
            return pltpu.make_async_copy(own[w], wholes[w].at[tuple(at)], local.at[w, 1])

        def first():
            for w in weights:
                take(w).start()
                for p in range(3):
                    copy(w, p, 0).start()
            for w in weights:
                for p in range(3):
                    relay(w, p, 0).start()
                take(w).wait()
                put(w).start()

        def later(w, stage):
            if stage == 1:
                put(w).wait()
            for p in range(3):
                copy(w, p, stage - 1).wait_recv()
                if stage < 3:
                    copy(w, p, stage).start()
                relay(w, p, stage).start()

        def last():
            for w in weights:
                for p in range(3):
                    for stage in range(4):
                        relay(w, p, stage).wait_recv()
                        relay(w, p, stage).wait_send()
                        if stage < 3:
                            copy(w, p, stage).wait_send()

        middle = [functools.partial(later, w, stage) for stage in (1, 2, 3) for w in weights]
        return [first, *middle, last]


class Scatter:
    def __init__(self, *terms):
        n = self.n = len(terms)
        terms, self.shifts, results, self.layers, self.starts = zip(*terms)
        so_far = [w for w in range(n) if not isinstance(results[w], jax.ShapeDtypeStruct)]
        self.inputs = [*terms, *[results[w] for w in so_far]]
        self.aliases = {n + k: w for k, w in enumerate(so_far)}
        shapes = [t.shape[4:] for t in terms]
        self.cols = [PARTS[s[1]] for s in shapes]
        self.rows = [s[0] for s in shapes]
        self.out_shapes = [jax.ShapeDtypeStruct(r.shape, BF16) for r in results]
        dma = pltpu.SemaphoreType.DMA
        self.scratch = []
        for s in shapes:
            self.scratch += [pltpu.VMEM((*(2,) * lead, *s), BF16) for lead in (3, 3, 2, 1, 0)]
        self.scratch += [dma((n, 2)), dma((n, 3, 4)), dma((n, 3, 3)), dma((n, 3, 3))]

    def order(self, w, p):
        return ORDERS[(p + self.shifts[w]) % 3]

    def events(self, terms, sums, scratch):
        held = [scratch[5 * w : 5 * w + 5] for w in range(self.n)]
        local, core, send, recv = scratch[5 * self.n :]
        at = place()
        cube = at[:3]
        items = [(w, p) for w in range(self.n) for p in range(3)]

        def swap(w, p, near):
            first = self.order(w, p)[0]
            index = [BOTH, BOTH, BOTH]
            index[first] = cube[first] if near else 1 - cube[first]
            src = terms[w].at[(*index, 1 - at[3], slice(None), columns(w, p))]
            dst = held[w][1].at[(*index, slice(None), columns(w, p))]
            return remote(src, dst, core.at[w, p, 2 * near], core.at[w, p, 2 * near + 1], 3)

        def take(w):
            return pltpu.make_async_copy(terms[w].at[BOTH, BOTH, BOTH, at[3]], held[w][0], local.at[w, 0])

        def put(w):
            mine = held[w][0].at[tuple(cube)]
            where = (self.layers[w], slice(None), pl.ds(self.starts[w], mine.shape[1]))
            return pltpu.make_async_copy(mine, sums[w].at[where], local.at[w, 1])

        def columns(w, p):
            return pl.ds(*self.cols[w][p])

        def copy(w, p, stage):
            order = self.order(w, p)
            index = list(cube)
            index[order[stage]] = 1 - cube[order[stage]]
            for a in order[stage + 1 :]:
                index[a] = BOTH
            src = held[w][0].at[(*index, slice(None), columns(w, p))]
            dst = held[w][2 + stage].at[(*(BOTH,) * (2 - stage), slice(None), columns(w, p))]
            return remote(src, dst, send.at[w, p, stage], recv.at[w, p, stage], order[stage])

        def add(w, p, stage):
            order = self.order(w, p)
            free = order[stage + 1 :] if stage < 3 else ()
            indices = []
            for number in range(2 ** len(free)):
                index = list(cube)
                if stage < 3:
                    index[order[stage]] = 1 - cube[order[stage]]
                for k, a in enumerate(free):
                    index[a] = (number >> k) & 1
                indices.append(index)

            def some_rows(i):
                where = (pl.ds(pl.multiple_of(i * 16, 16), 16), columns(w, p))
                totals = []
                for index in indices:
                    total = held[w][0][(*index, *where)].astype(F32) + held[w][1][(*index, *where)].astype(F32)
                    for j in range(stage):
                        rest = [index[a] for a in range(3) if a not in order[: j + 1]]
                        total += held[w][2 + j][(*rest, *where)].astype(F32)
                    totals.append(total.astype(BF16))
                for index, total in zip(indices, totals):
                    held[w][0][(*index, *where)] = total

            pl.loop(0, self.rows[w] // 16)(some_rows)

        def first():
            for near in (0, 1):
                for w in range(self.n):
                    for p in range(3):
                        swap(w, p, near).start()
                    if not near:
                        take(w).start()

        def leave(w, stage):
            if stage == 0:
                take(w).wait()
            for p in range(3):
                if stage < 2:
                    swap(w, p, stage).wait_recv()
                if stage > 0:
                    copy(w, p, stage - 1).wait_recv()
                add(w, p, stage)
                if stage < 3:
                    copy(w, p, stage).start()
            if stage == 3:
                put(w).start()

        def last():
            for w in range(self.n):
                for p in range(3):
                    swap(w, p, 0).wait_send()
                    swap(w, p, 1).wait_send()
                    for stage in range(3):
                        copy(w, p, stage).wait_send()
                put(w).wait()

        middle = [functools.partial(leave, w, stage) for stage in range(4) for w in range(self.n)]
        return [first, *middle, last]


def call(name, body, steps, inputs, in_specs, out_shapes, out_specs, flops=0, late=(), scratch=(), aliases=None, side=None, when=(), number=None):
    n_in, n_out, n_scratch = len(inputs), len(out_shapes), len(scratch)
    s_in, s_out = (len(side.inputs), len(side.out_shapes)) if side else (0, 0)
    n_late = len(late)

    def kernel(*refs):
        ins, refs = refs[:n_in], refs[n_in:]
        side_ins, refs = refs[:s_in], refs[s_in:]
        late_ins, refs = refs[:n_late], refs[n_late:]
        outs, refs = refs[:n_out], refs[n_out:]
        side_outs, refs = refs[:s_out], refs[s_out:]
        own, refs = refs[:n_scratch], refs[n_scratch:]
        held, refs = refs[:n_late], refs[n_late:]
        (late_sem, side_scratch) = (refs[0], refs[1:]) if late else (None, refs)
        step = pl.program_id(0)

        def fetch(k):
            return pltpu.make_async_copy(late_ins[k], held[k], late_sem.at[k])

        def ready(k):
            pl.when(step == 0)(lambda: fetch(k).wait())

        if late:

            def fetch_all():
                for k in range(n_late):
                    fetch(k).start()

            pl.when(step == 0)(fetch_all)
        events = side.events(side_ins, side_outs, side_scratch) if side else []
        for k, event in enumerate(events):
            if k < len(when):

                def now(event=event, k=k):
                    if k == 0:
                        meet()
                    event()

                pl.when(step == when[k])(now)
        body(*ins, *outs, *own, *((held, ready) if late else ()))
        if len(events) > len(when):

            def end():
                for event in events[len(when) :]:
                    event()

            pl.when(step == steps - 1)(end)

    params = dict(vmem_limit_bytes=VMEM_LIMIT, dimension_semantics=("arbitrary",))
    if side:
        params |= dict(collective_id=number, has_side_effects=True)
    return pl.pallas_call(
        kernel,
        name=name,
        grid=(steps,),
        in_specs=[*in_specs, *[ANY] * (s_in + n_late)],
        out_specs=[*out_specs, *[ANY] * s_out],
        out_shape=[*out_shapes, *(side.out_shapes if side else ())],
        scratch_shapes=[
            *scratch,
            *[pltpu.VMEM(a.shape, a.dtype) for a in late],
            *([pltpu.SemaphoreType.DMA((n_late,))] if late else []),
            *(side.scratch if side else ()),
        ],
        input_output_aliases={**(aliases or {}), **({n_in + i: n_out + o for i, o in side.aliases.items()} if side else {})},
        compiler_params=pltpu.CompilerParams(**params),
        cost_estimate=pl.CostEstimate(flops=flops, bytes_accessed=0, transcendentals=0),
    )(*inputs, *(side.inputs if side else ()), *late)


def shape(*dims, dtype=BF16):
    return jax.ShapeDtypeStruct(dims, dtype)


def kept(*dims):
    return pl.BlockSpec(dims, lambda i: (0,) * len(dims), pipeline_mode=pl.Buffered(1))


def across(rows, size):
    return pl.BlockSpec((rows, size), lambda i: (0, i))


def down(size, cols):
    return pl.BlockSpec((size, cols), lambda i: (i, 0))


T, D, FF = 2048, 1024, 2816
MM = 2 * T * D * FF


def scale_of(wide):
    return lax.rsqrt(jnp.mean(wide**2, -1, keepdims=True) + EPS)


def normed(wide):
    return (wide * scale_of(wide)).astype(BF16)


def norm_body(x, a, at):
    wide = x[...].astype(F32)
    y = wide * scale_of(wide)
    a[...] = y.astype(BF16)
    at[...] = y.T.astype(BF16)


def norm(x, **side):
    n = 256
    return call("norm", norm_body, T // n, [x], [down(n, D)], [shape(T, D), shape(D, T)], [down(n, D), across(D, n)], **side)


def chunks(n=512):
    return [pl.ds(r, n) for r in range(0, T, n)]


def gate_up_body(a, wg, wu, gate, up, hid):
    for r in chunks():
        g, u = dot(a[r, :], wg[...]), dot(a[r, :], wu[...])
        gate[r, :], up[r, :] = g, u
        hid[r, :] = (g * jax.nn.sigmoid(g) * u).astype(BF16)


def gate_up(a, wg, wu, **side):
    n = 256
    wide = shape(T, FF, dtype=F32)
    return call(
        "gate_up", gate_up_body, FF // n, [a, wg, wu], [kept(T, D), across(D, n), across(D, n)],
        [wide, wide, shape(T, FF)], [across(T, n)] * 3, flops=2 * MM, **side,
    )


def down_body(hid, wd, x, h, a, at):
    y = x[...] + dot(hid[...], wd[...]).astype(BF16)
    h[...] = y
    wide = y.astype(F32)
    y = wide * scale_of(wide)
    a[...] = y.astype(BF16)
    at[...] = y.T.astype(BF16)


def down_norm(hid, wd, x, **side):
    n = 256
    return call(
        "down", down_body, T // n, [hid, wd, x], [down(n, FF), kept(FF, D), down(n, D)],
        [shape(T, D), shape(T, D), shape(D, T)], [down(n, D), down(n, D), across(D, n)], flops=MM, **side,
    )


def gated_back(g, u, d):
    s = jax.nn.sigmoid(g)
    gs = g * s
    return (d * u * (s + gs * (1 - s))).astype(BF16), (d * gs).astype(BF16), (gs * u).astype(BF16)


def grads(r_at, r_dy, dgate, dup, hid, gd, gg, gu):
    gg[...] = dot(r_at[...], dgate[...]).astype(BF16)
    gu[...] = dot(r_at[...], dup[...]).astype(BF16)
    gd[...] = dot(hid[...], r_dy[...], TN).astype(BF16)


def turn_body(a, wg, wu, wd, *refs):
    *_, dgate, dup, gd, gg, gu, hid, (dy, at), ready = refs
    ready(0)
    for r in chunks(256):
        g, u = dot(a[r, :], wg[...]), dot(a[r, :], wu[...])
        d = dot(dy[r, :], wd[...], NT).astype(BF16).astype(F32)
        dgate[r, :], dup[r, :], hid[r, :] = gated_back(g, u, d)
    ready(1)
    grads(at, dy, dgate, dup, hid, gd, gg, gu)


def turn(a, at, dy, wg, wu, wd, first, tiles, so_far=(), **side):
    n = 256
    columns = pl.BlockSpec((T, n), lambda i: (0, first + i))
    rows = pl.BlockSpec((n, D), lambda i: (first + i, 0))
    return call(
        f"turn_{first}", turn_body, tiles, [a, wg, wu, wd, *so_far],
        [kept(T, D), across(D, n), across(D, n), rows, *[ANY] * len(so_far)],
        [shape(T, FF), shape(T, FF), shape(FF, D), shape(D, tiles * n), shape(D, tiles * n)],
        [columns, columns, rows, across(D, n), across(D, n)],
        flops=6 * MM * tiles // 11, scratch=[pltpu.VMEM((T, n), BF16)], late=[dy, at],
        aliases={4 + k: k for k in range(len(so_far))}, **side,
    )


def hidden_back_body(dh, wd, gate, up, *refs):
    *_, dgate, dup, gd, gg, gu, hid, (at,), ready = refs

    @pl.loop(0, 2)
    def half(i):
        r = pl.ds(pl.multiple_of(i * (T // 2), T // 2), T // 2)
        d = dot(dh[r, :], wd[...], NT).astype(BF16).astype(F32)
        dgate[r, :], dup[r, :], hid[r, :] = gated_back(gate[r, :], up[r, :], d)

    ready(0)
    grads(at, dh, dgate, dup, hid, gd, gg, gu)


def hidden_back(at, dh, wd, gate, up, first, tiles, so_far=(), **side):
    n = 256
    columns = pl.BlockSpec((T, n), lambda i: (0, first + i))
    rows = pl.BlockSpec((n, D), lambda i: (first + i, 0))
    return call(
        f"hidden_back_{first}", hidden_back_body, tiles, [dh, wd, gate, up, *so_far],
        [kept(T, D), rows, columns, columns, *[ANY] * len(so_far)],
        [shape(T, FF), shape(T, FF), shape(FF, D), shape(D, tiles * n), shape(D, tiles * n)],
        [columns, columns, rows, across(D, n), across(D, n)],
        flops=4 * MM * tiles // 11, scratch=[pltpu.VMEM((T, n), BF16)], late=[at],
        aliases={4 + k: k for k in range(len(so_far))}, **side,
    )


def back_body(dg, du, h, dy, out, weights, ready):
    pieces = len(weights) // 2
    for k, w in enumerate(weights):
        if k % pieces == 0:
            start = 0
        d = (dg, du)[k // pieces][:, start : start + w.shape[1]]
        start += w.shape[1]
        ready(k)
        da = dot(d, w[...], NT) + (da if k else 0)
    da = da.astype(BF16).astype(F32)
    wide = h[...].astype(F32)
    s = scale_of(wide)
    through = jnp.sum(da * wide, -1, keepdims=True)
    out[...] = dy[...] + (da * s - wide * (s * s * s * through / D)).astype(BF16)


def back(dg, du, wg, wu, h, dy, **side):
    n = 256
    return call(
        "back", back_body, T // n, [dg, du, h, dy], [down(n, FF), down(n, FF), down(n, D), down(n, D)],
        [shape(T, D)], [down(n, D)], late=[*wg, *wu], flops=2 * MM, **side,
    )


def blocks_of(grad):
    return grad.reshape(2, 2, 2, 2, -1, grad.shape[-1])


def device_step(x, dy, w_gate, w_up, w_down):
    x, dy = x.reshape(T, D), dy.reshape(T, D)

    a0, a0t, wg0, wu0 = norm(x, side=Gather((w_gate, 0, 0, FF, 0), (w_up, 0, 0, FF, 1)), when=(0, 3, 5), number=1)
    wg0, wu0 = wg0.reshape(D, FF), wu0.reshape(D, FF)
    grad = shape(2, D // 16, FF)
    first, rest = 1280, 1536
    gate0, up0, hid0, wd0, wg1a = gate_up(
        a0, wg0, wu0, side=Gather((w_down, 0, 0, D, 0), (w_gate, 1, 0, first, 2)), when=(0, 1, 2, 4, 5, 9), number=2
    )
    wd0, wg1a = wd0.reshape(FF, D), wg1a.reshape(D, first)
    h1, a1, a1t, wd1, wu1a = down_norm(
        hid0, wd0, x, side=Gather((w_down, 1, 0, D, 0), (w_up, 1, 0, first, 2)), when=(0, 2, 2, 4, 6), number=3
    )
    wd1, wu1a = wd1.reshape(FF, D), wu1a.reshape(D, first)

    *so_far, gg1a, gu1a, wg1b, wu1b = turn(
        a1, a1t, dy, wg1a, wu1a, wd1, 0, 5,
        side=Gather((w_gate, 1, first, rest, 0), (w_up, 1, first, rest, 1)), when=(0, 1, 1, 2, 2, 4, 4), number=4,
    )
    wg1b, wu1b = wg1b.reshape(D, rest), wu1b.reshape(D, rest)
    dgate1, dup1, gd1, gg1b, gu1b, sg, su = turn(
        a1, a1t, dy, wg1b, wu1b, wd1, 5, 6, so_far,
        side=Scatter((blocks_of(gg1a), 0, grad, 1, 0), (blocks_of(gu1a), 1, grad, 1, 0)), when=(0, 1, 1, 3, 3, 4, 4, 5, 5), number=5,
    )
    dh1, sd = back(
        dgate1, dup1, [wg1a, wg1b], [wu1a, wu1b], h1, dy,
        side=Scatter((blocks_of(gd1), 0, shape(2, FF // 16, D), 1, 0)), when=(0, 1, 4, 6, 7), number=6,
    )
    *so_far, gg0a, gu0a, sg, su = hidden_back(
        a0t, dh1, wd0, gate0, up0, 0, 6,
        side=Scatter((blocks_of(gg1b), 0, sg, 1, first), (blocks_of(gu1b), 1, su, 1, first)),
        when=(0, 1, 1, 3, 3, 4, 4, 5, 5), number=7,
    )
    dgate0, dup0, gd0, gg0b, gu0b, sg, su = hidden_back(
        a0t, dh1, wd0, gate0, up0, 6, 5, so_far,
        side=Scatter((blocks_of(gg0a), 0, sg, 0, 0), (blocks_of(gu0a), 1, su, 0, 0)), when=(0, 1, 1, 3, 3, 4, 4), number=8,
    )
    half = 6 * 256
    dx, sd, sg, su = back(
        dgate0, dup0, [wg0], [wu0], x, dh1,
        side=Scatter((blocks_of(gd0), 0, sd, 0, 0), (blocks_of(gg0b), 2, sg, 0, half), (blocks_of(gu0b), 2, su, 0, half)),
        when=(0, 1, 1, 2, 4, 5, 6), number=9,
    )
    return dx[None], sg, su, sd


def solution(mesh):
    tokens, rows = P(("rep", "dp"), None, None), P(None, "dp", None)
    return jax.shard_map(
        device_step,
        mesh=mesh,
        in_specs=(tokens, tokens, rows, rows, rows),
        out_specs=(tokens, P("rep", "dp", None), P("rep", "dp", None), P("rep", "dp", None)),
        check_vma=False,
    )
```
